128 devices in a mesh: row: 8 (over z, y_hi), col: 16 (over x, y_lo, core).
Axes of the slice: x: 4, y: 4 (y_hi: 2, y_lo: 2; y = y_hi * 2 + y_lo), z: 4, core: 2. Of those that a mesh axis runs over, the one named last changes fastest.
Arguments:
- tokens_in: bfloat16 [16384, 1408], P(('row', 'col')), may hold values from -300 to 300
- ln1_gain: bfloat16 [1408], replicated, may hold values from 0.099609375 to 1.8984375
- ln1_bias: bfloat16 [1408], replicated, may hold values from -3 to 3
- qkv_weight: bfloat16 [1408, 4224], P('row', 'col'), may hold values from -0.8 to 0.8
- qkv_bias: bfloat16 [4224], P('col'), may hold values from -3 to 3
- proj_weight: bfloat16 [1408, 1408], P('col', 'row'), may hold values from -0.15625 to 0.15625
- proj_bias: bfloat16 [1408], replicated, may hold values from -3 to 3
- ln2_gain: bfloat16 [1408], replicated, may hold values from 0.099609375 to 1.8984375
- ln2_bias: bfloat16 [1408], replicated, may hold values from -3 to 3
- fc1_weight: bfloat16 [1408, 6144], P('row', 'col'), may hold values from -0.15625 to 0.15625
- fc1_bias: bfloat16 [6144], P('col'), may hold values from -3 to 3
- fc2_weight: bfloat16 [1408, 6144], P('row', 'col'), may hold values from -0.078125 to 0.078125
- fc2_bias: bfloat16 [1408], replicated, may hold values from -3 to 3
Outputs:
- tokens_out: bfloat16 [16384, 1408], P(('row', 'col'))
The draws below stay inside these ranges and needn't reach their ends.
All inputs are finite; a program needn't handle non-finite values.
Results may differ from the reference program's by a relative error of at most 0.01.
Values may be sent and summed in bfloat16 or wider, within the bound.
A program may use at most 64 MiB of HBM per device.

```python
import jax
import jax.numpy as jnp
from jax import lax

D = 1408
HEADS = 16
FF = 6144
LEN = 2048
TOKENS = 16384
N_ROW = 8
N_COL = 16


def draw_tokens_in(key, part):
    key_base = jax.random.fold_in(key, 11)
    columns = 1.0 + 2.0 * jnp.arange(D, dtype=jnp.float32) / (D - 1)
    base = jax.random.normal(key_base, (TOKENS, D), jnp.float32)
    return (base * columns).astype(jnp.bfloat16)


def draw_qkv_weight(key, part):
    noise = jax.random.normal(jax.random.fold_in(key, 21), (D, 3 * D), jnp.float32) * D ** (-0.5)
    return jnp.clip(noise, -0.8, 0.8).astype(jnp.bfloat16)


def shard_levels(stream_key, dims, cuts, low, largest):
    level, own = 1.0, jax.random.fold_in(stream_key, 6)
    for position, shards_of in cuts:
        draws = jnp.exp(jax.random.uniform(jax.random.fold_in(own, position), (shards_of,), jnp.float32, low / len(cuts), largest / len(cuts)))
        level = level * jnp.repeat(draws, dims[position] // shards_of).reshape([-1 if axis == position else 1 for axis in range(len(dims))])
    return level


def normal_values(own_key, dims, spread, reach, pieces=(), held_as=jnp.bfloat16):
    level = shard_levels(own_key, dims, pieces, -0.22, 0.18) if pieces else 1.0
    drawn = jax.random.normal(own_key, dims, jnp.float32) * spread * level
    return jnp.minimum(jnp.maximum(drawn, -reach), reach).astype(held_as)


def setup_inputs(seed: int = 0) -> dict:
    streams_of = jax.random.split(jax.random.key(seed), 14)
    return {
        "tokens_in": draw_tokens_in(jax.random.fold_in(streams_of[13], 71), 0),
        "ln1_gain": jnp.clip(1.0 + 0.18 * jax.random.normal(streams_of[1], (D,), jnp.float32), 0.099609375, 1.8984375).astype(jnp.bfloat16),
        "ln1_bias": normal_values(streams_of[2], (D,), 0.5, 3.0),
        "qkv_weight": draw_qkv_weight(jax.random.fold_in(streams_of[13], 71), 0),
        "qkv_bias": normal_values(streams_of[4], (3 * D,), 0.5, 3.0, ((0, 16),)),
        "proj_weight": normal_values(streams_of[5], (D, D), D ** -0.5, 0.15625, ((0, 16), (1, 8))),
        "proj_bias": normal_values(streams_of[6], (D,), 0.5, 3.0),
        "ln2_gain": jnp.clip(1.0 + 0.18 * jax.random.normal(streams_of[7], (D,), jnp.float32), 0.099609375, 1.8984375).astype(jnp.bfloat16),
        "ln2_bias": normal_values(streams_of[8], (D,), 0.5, 3.0),
        "fc1_weight": normal_values(streams_of[9], (D, FF), D ** -0.5, 0.15625, ((0, 8), (1, 16))),
        "fc1_bias": normal_values(streams_of[10], (FF,), 0.5, 3.0, ((0, 16),)),
        "fc2_weight": normal_values(streams_of[11], (D, FF), FF ** -0.5, 0.078125, ((0, 8), (1, 16))),
        "fc2_bias": normal_values(streams_of[12], (D,), 0.5, 3.0),
    }


def layer_norm(values, gain, bias):
    mean = lax.optimization_barrier(jnp.mean(values, axis=-1, keepdims=True))
    centred = values - mean
    var = lax.optimization_barrier(jnp.mean(centred * centred, axis=-1, keepdims=True))
    return centred * lax.rsqrt(var + 1e-06) * gain.astype(jnp.float32) + bias.astype(jnp.float32)

def attend(qkv, heads):
    length = qkv.shape[0]
    head_size = qkv.shape[1] // (3 * heads)
    parts = qkv.reshape(length, heads, 3, head_size).astype(jnp.float32)
    query = parts[:, :, 0]
    keys = parts[:, :, 1]
    values = parts[:, :, 2]
    block = min(512, length)
    blocks = query.reshape(length // block, block, heads, head_size)
    scale = 1.0 / head_size ** 0.5

    def one_block(qblock):
        scores = jnp.einsum('qhe,khe->hqk', qblock, keys) * scale
        top = lax.optimization_barrier(jnp.max(scores, axis=-1, keepdims=True))
        expo = jnp.exp(scores - top)
        probs = (expo / lax.optimization_barrier(jnp.sum(expo, axis=-1, keepdims=True))).astype(jnp.bfloat16)
        mixed = jnp.einsum('hqk,khe->qhe', probs.astype(jnp.float32), values)
        return mixed.astype(jnp.bfloat16).reshape(block, heads * head_size)
    return lax.map(one_block, blocks).reshape(length, heads * head_size)

def grouped_sum(left, right, groups):
    width = left.shape[1] // groups
    lefts = left.reshape(left.shape[0], groups, width).transpose(1, 0, 2)
    rights = right.reshape(groups, width, right.shape[1])

    def add_group(total, pair):
        part = jnp.dot(pair[0], pair[1], preferred_element_type=jnp.float32).astype(jnp.bfloat16)
        part = lax.optimization_barrier(part)
        return (total + part.astype(jnp.float32), None)
    start = jnp.zeros((left.shape[0], right.shape[1]), jnp.float32)
    total, _ = lax.scan(add_group, start, (lefts, rights))
    return total

def reference(tokens_in, ln1_gain, ln1_bias, qkv_weight, qkv_bias, proj_weight, proj_bias, ln2_gain, ln2_bias, fc1_weight, fc1_bias, fc2_weight, fc2_bias):
    inputs = tokens_in.astype(jnp.float32)
    ln1 = layer_norm(inputs, ln1_gain, ln1_bias).astype(jnp.bfloat16)
    qkv = jnp.dot(ln1, qkv_weight, preferred_element_type=jnp.float32) + qkv_bias.astype(jnp.float32)
    qkv = qkv.astype(jnp.bfloat16)
    clips = qkv.reshape(N_ROW, LEN, 3 * D)
    attn = lax.map(lambda clip: attend(clip, HEADS), clips).reshape(TOKENS, D)
    resid = inputs + grouped_sum(attn, proj_weight, N_COL) + proj_bias.astype(jnp.float32)
    ln2 = layer_norm(resid, ln2_gain, ln2_bias).astype(jnp.bfloat16)
    hidden = jnp.dot(ln2, fc1_weight, preferred_element_type=jnp.float32) + fc1_bias.astype(jnp.float32)
    hidden = jax.nn.gelu(hidden, approximate=False).astype(jnp.bfloat16)
    result = resid + grouped_sum(hidden, fc2_weight.T, N_COL) + fc2_bias.astype(jnp.float32)
    return result.astype(jnp.bfloat16)
```

```python
import jax
import jax.numpy as jnp
from jax import lax
from jax.experimental import pallas as pl
from jax.experimental.pallas import tpu as pltpu
from jax.sharding import PartitionSpec as P

MESH = pl.DeviceIdType.MESH
F32 = jnp.float32
BF16 = jnp.bfloat16
D = 1408
HEAD = 88
COPIES = 96
SCALE = (1.0 / HEAD**0.5) * 1.4426950408889634
NT = (((1,), (1,)), ((), ()))


def norm(values, gain, bias):
    mean = jnp.mean(values, axis=-1, keepdims=True)
    centred = values - mean
    var = jnp.mean(centred * centred, axis=-1, keepdims=True)
    return centred * lax.rsqrt(var + 1e-06) * gain + bias


def kernel(
    tok, prm, wq, wp, f1, f2, out,
    X, WQ, WP, F1, F2, FB, QKV, O, OA, RES, H, PART, SS, SD, KEEP, D2S, PS, MS, RA, RB, RL, RR,
    send, recv, asend, arecv, lsem,
):
    r = lax.axis_index("row")
    c = lax.axis_index("col")
    z, yh = r // 2, r % 2
    x, yl, core = c // 4, (c // 2) % 2, c % 2
    y = yh * 2 + yl
    chip = c // 2

    def plus(v, n):
        return lax.rem(v + n, 4)

    def at_x(v):
        return (r, v * 4 + yl * 2 + core)

    def at_y(v):
        return (z * 2 + v // 2, x * 4 + lax.rem(v, 2) * 2 + core)

    def at_z(v):
        return (v * 2 + yh, c)

    xp, xm = at_x(plus(x, 1)), at_x(plus(x, 3))
    yp, ym = at_y(plus(y, 1)), at_y(plus(y, 3))
    zp, zm = at_z(plus(z, 1)), at_z(plus(z, 3))
    ylp = (r, x * 4 + (1 - yl) * 2 + core)
    yh2 = (z * 2 + 1 - yh, c)
    dd = (r, x * 4 + yl * 2 + 1 - core)

    barrier = pltpu.get_barrier_semaphore()
    for peer in (yp, ym, zp, zm, yh2):
        pl.semaphore_signal(barrier, inc=1, device_id=peer, device_id_type=MESH)

    def greet(i, carry):
        pl.semaphore_signal(
            barrier, inc=1, device_id=(r, lax.rem(c + i, 16)), device_id_type=MESH
        )
        return carry

    lax.fori_loop(1, 16, greet, 0)

    def cols(v):
        return pl.ds(pl.multiple_of(v * 384, 384), 384)

    def lanes(xv, ylv, cv):
        return pl.ds(pl.multiple_of(cv * 1024 + xv * 256 + ylv * 128, 128), 128)

    def wide(xv):
        return pl.ds(pl.multiple_of(core * 1024 + xv * 256, 256), 256)

    loads = [
        pltpu.make_async_copy(wq, WQ.at[z, yh], lsem.at[0]),
        pltpu.make_async_copy(f1, F1.at[z, yh, :, cols(yl)], lsem.at[1]),
        pltpu.make_async_copy(f2, F2.at[z, yh, :, cols(yl)], lsem.at[2]),
        pltpu.make_async_copy(wp, WP.at[z, yh, :, lanes(x, yl, core)], lsem.at[3]),
    ]
    for load in loads:
        load.start()

    started = []

    def go(src, dst, dev):
        i = len(started)
        copy = pltpu.make_async_remote_copy(
            src_ref=src, dst_ref=dst, send_sem=send.at[i], recv_sem=recv.at[i],
            device_id=dev, device_id_type=MESH,
        )
        copy.start()
        started.append(copy)
        return copy

    def push(ref, dev):
        return go(ref, ref, dev)

    inputs = tok[...].astype(F32)
    X[chip, core] = norm(inputs, prm[0:1, :], prm[1:2, :]).astype(BF16)
    FB[yl] = jnp.broadcast_to(prm[6:7, 384:768], (8, 384))
    for load in loads:
        load.wait()
    pl.semaphore_wait(barrier, 20)

    own = X.at[chip, core]
    wq_own = WQ.at[z, yh]
    q_y2 = push(wq_own, yh2)
    q_p = push(wq_own, zp)
    q_m = push(wq_own, zm)
    a_p = push(own, xp)
    a_m = push(own, xm)
    a_y = push(own, ylp)
    a_d = push(own, dd)
    b_y = push(FB.at[yl], ylp)

    def f_piece(F, zv, yv):
        return F.at[zv, yv // 2, :, cols(lax.rem(yv, 2))]

    def f_half(F, zv, yv, first):
        rows = pl.ds(0, 96) if first else pl.ds(96, 80)
        return F.at[zv, yv // 2, rows, cols(lax.rem(yv, 2))]

    def p_half(yv, first):
        rows = pl.ds(0, 96) if first else pl.ds(96, 80)
        return WP.at[z, yv // 2, rows, lanes(x, lax.rem(yv, 2), core)]

    p_own = WP.at[z, yh, :, lanes(x, yl, core)]
    py_p = push(p_own, yp)
    py_m = push(p_own, ym)
    f2z_p = push(f_piece(F2, z, y), zp)
    f2z_m = push(f_piece(F2, z, y), zm)
    f1y_p = push(f_piece(F1, z, y), yp)
    f1y_m = push(f_piece(F1, z, y), ym)

    q_y2.wait_recv()
    wq_other = WQ.at[z, 1 - yh]
    q2_p = push(wq_other, zp)
    q2_m = push(wq_other, zm)
    q_p.wait_recv()
    q_pf = push(WQ.at[plus(z, 3), yh, pl.ds(0, 96)], zp)
    q_m.wait_recv()
    q_mf = push(WQ.at[plus(z, 1), yh, pl.ds(96, 80)], zm)

    def chip_of(xv, ylv):
        return xv * 2 + ylv

    left, right, far = plus(x, 3), plus(x, 1), plus(x, 2)
    a_p.wait_recv()
    l1 = X.at[chip_of(left, yl), core]
    a_pf = push(X.at[chip_of(left, yl), core, pl.ds(0, 64)], xp)
    l1_d = push(l1, dd)
    a_m.wait_recv()
    r1 = X.at[chip_of(right, yl), core]
    a_mf = push(X.at[chip_of(right, yl), core, pl.ds(64, 64)], xm)
    r1_d = push(r1, dd)
    a_y.wait_recv()
    p0 = X.at[chip_of(x, 1 - yl), core]
    y_p = push(p0, xp)
    y_m = push(p0, xm)
    p0_d = push(p0, dd)

    q2_p.wait_recv()
    q2_pf = push(WQ.at[plus(z, 3), 1 - yh, pl.ds(0, 96)], zp)
    q2_m.wait_recv()
    q2_mf = push(WQ.at[plus(z, 1), 1 - yh, pl.ds(96, 80)], zm)

    def qkv(where):
        block = X[where].reshape(256, D)
        product = jnp.dot(block, WQ[...].reshape(D, 384), preferred_element_type=F32)
        QKV[where] = (product + prm[6:7, 0:384]).astype(BF16)

    a_pf.wait_recv()
    a_mf.wait_recv()
    d2 = X.at[chip_of(far, yl), core]
    d2_y = push(d2, ylp)
    d2_d = push(d2, dd)

    py_p.wait_recv()
    py_pf = push(p_half(plus(y, 3), True), yp)
    py_m.wait_recv()
    py_mf = push(p_half(plus(y, 1), False), ym)
    f2z_p.wait_recv()
    f2z_pf = push(f_half(F2, plus(z, 3), y, True), zp)
    f2z_m.wait_recv()
    f2z_mf = push(f_half(F2, plus(z, 1), y, False), zm)
    f1y_p.wait_recv()
    f1y_pf = push(f_half(F1, z, plus(y, 3), True), yp)
    f1y_m.wait_recv()
    f1y_mf = push(f_half(F1, z, plus(y, 1), False), ym)

    for copy in (q_pf, q_mf, q2_pf, q2_mf, a_d):
        copy.wait_recv()
    qkv(chip)
    l1_d.wait_recv()
    qkv(chip_of(left, yl))
    r1_d.wait_recv()
    qkv(chip_of(right, yl))
    p0_d.wait_recv()
    qkv(chip_of(x, 1 - yl))

    py_pf.wait_recv()
    py_mf.wait_recv()
    p_zown = WP.at[z, :, :, wide(x)]
    pz_p = push(p_zown, zp)
    pz_m = push(p_zown, zm)

    d2_d.wait_recv()
    qkv(chip_of(far, yl))

    y_p.wait_recv()
    pl1 = X.at[chip_of(left, 1 - yl), core]
    pl1_d = push(pl1, dd)
    y_m.wait_recv()
    pr1 = X.at[chip_of(right, 1 - yl), core]
    pr1_d = push(pr1, dd)
    d2_y.wait_recv()
    pd2 = X.at[chip_of(far, 1 - yl), core]
    pd2_d = push(pd2, dd)

    f2z_pf.wait_recv()
    f2z_mf.wait_recv()
    f2_yown = F2.at[:, yh, :, cols(yl)]
    f2y_p = push(f2_yown, yp)
    f2y_m = push(f2_yown, ym)
    f1y_pf.wait_recv()
    f1y_mf.wait_recv()
    f1_zown = F1.at[z]
    f1z_p = push(f1_zown, zp)
    f1z_m = push(f1_zown, zm)
    pz_p.wait_recv()
    pz_pf = push(WP.at[plus(z, 3), 0, :, wide(x)], zp)
    pz_m.wait_recv()
    pz_mf = push(WP.at[plus(z, 1), 1, :, wide(x)], zm)

    pl1_d.wait_recv()
    qkv(chip_of(left, 1 - yl))
    pr1_d.wait_recv()
    qkv(chip_of(right, 1 - yl))
    pd2_d.wait_recv()
    qkv(chip_of(far, 1 - yl))

    def attend(tc):
        q = QKV[tc, :, 0:128]
        k = QKV[:, :, 128:256].reshape(2048, 128)
        v = QKV[:, :, 256:384].reshape(2048, 128)
        s = lax.dot_general(q, k, NT, preferred_element_type=F32)
        top = jnp.max(s, axis=-1, keepdims=True)
        p = jnp.exp2((s - top) * SCALE).astype(BF16)
        mixed = jnp.dot(p, v, preferred_element_type=F32)
        o = (mixed / mixed[:, HEAD : HEAD + 1]).astype(BF16)
        O[tc] = o.reshape(2, 128, 128)

    slot = lanes(x, yl, core)

    def away(tc, i, other):
        return pltpu.make_async_remote_copy(
            src_ref=O.at[tc, other], dst_ref=OA.at[:, slot],
            send_sem=asend.at[i * 2 + other], recv_sem=arecv.at[i * 2 + core],
            device_id=(r, tc * 2 + other), device_id_type=MESH,
        )

    def block(i, carry):
        tc = lax.rem(chip + i, 8)
        attend(tc)
        away(tc, i, 0).start()
        away(tc, i, 1).start()
        return carry

    lax.fori_loop(1, 2, block, 0)
    pz_pf.wait_recv()
    pz_mf.wait_recv()
    p_xown = WP.at[:, :, :, wide(x)]
    px_p = push(p_xown, xp)
    px_m = push(p_xown, xm)
    lax.fori_loop(2, 6, block, 0)
    f1z_p.wait_recv()
    f1z_pf = push(F1.at[plus(z, 3), 0], zp)
    f1z_m.wait_recv()
    f1z_mf = push(F1.at[plus(z, 1), 1], zm)
    f2y_p.wait_recv()
    yb, yf = plus(y, 3), plus(y, 1)
    f2y_pf = push(F2.at[pl.ds(0, 2), yb // 2, :, cols(lax.rem(yb, 2))], yp)
    f2y_m.wait_recv()
    f2y_mf = push(F2.at[pl.ds(2, 2), yf // 2, :, cols(lax.rem(yf, 2))], ym)
    lax.fori_loop(6, 8, block, 0)
    px_p.wait_recv()
    px_pf = push(WP.at[pl.ds(0, 2), :, :, wide(left)], xp)
    px_m.wait_recv()
    px_mf = push(WP.at[pl.ds(2, 2), :, :, wide(right)], xm)
    attend(chip)
    home = pltpu.make_async_remote_copy(
        src_ref=O.at[chip, 1 - core], dst_ref=OA.at[:, slot],
        send_sem=asend.at[0], recv_sem=arecv.at[core],
        device_id=dd, device_id_type=MESH,
    )
    home.start()
    OA[:, slot] = O[chip, core]

    px_pf.wait_recv()
    px_mf.wait_recv()
    p_half_own = WP.at[:, :, :, pl.ds(pl.multiple_of(core * 1024, 1024), 1024)]
    p_d = push(p_half_own, dd)

    def arrived(i, other):
        pltpu.make_async_remote_copy(
            src_ref=O.at[0, 0], dst_ref=OA.at[:, slot],
            send_sem=asend.at[i * 2], recv_sem=arecv.at[i * 2 + other],
            device_id=dd, device_id_type=MESH,
        ).wait_recv()

    arrived(0, 1 - core)

    def arrivals(i, carry):
        arrived(i, 0)
        arrived(i, 1)
        return carry

    lax.fori_loop(1, 8, arrivals, 0)
    p_d.wait_recv()

    summed = lax.dot_general(OA[...], WP[...].reshape(D, 2048), NT, preferred_element_type=F32)
    resid = tok[...].astype(F32) + summed + prm[2:3, :]
    RES[...] = resid
    H[x, core] = norm(resid, prm[3:4, :], prm[4:5, :]).astype(BF16)

    h_own = H.at[x, core]
    h_p = push(h_own, xp)
    h_m = push(h_own, xm)
    h_d = push(h_own, dd)

    for copy in (f1z_pf, f1z_mf, f2y_pf, f2y_mf, b_y):
        copy.wait_recv()

    def mlp(k, where):
        h = H[where].reshape(256, D)
        a = jnp.dot(h, F1[...].reshape(D, 768), preferred_element_type=F32)
        a = a + jnp.concatenate([FB[0, 0:1, :], FB[1, 0:1, :]], axis=1)
        hidden = (0.5 * a * (1.0 + lax.erf(a * 0.7071067811865476))).astype(BF16)
        part = lax.dot_general(hidden, F2[...].reshape(D, 768), NT, preferred_element_type=F32)
        PART[k] = part.reshape(2, 128, D)
        SS[k] = PART[k, 1 - core].astype(BF16)
        return go(SS.at[k], SD.at[k], dd)

    h_d.wait_recv()
    s_own = mlp(0, x)
    h_p.wait_recv()
    h_pf = push(H.at[left, core, pl.ds(0, 64)], xp)
    hl_d = push(H.at[left, core], dd)
    h_m.wait_recv()
    h_mf = push(H.at[right, core, pl.ds(64, 64)], xm)
    hr_d = push(H.at[right, core], dd)
    hl_d.wait_recv()
    s_l = mlp(1, left)
    hr_d.wait_recv()
    s_r = mlp(2, right)
    h_pf.wait_recv()
    h_mf.wait_recv()
    hf_d = push(H.at[far, core], dd)

    top, low = slice(0, 64), slice(64, 128)
    s_l.wait_recv()
    total = PART[1, core] + SD[1].astype(F32)
    MS[top] = total[top].astype(BF16)
    KEEP[1] = total[low]
    m_a = go(MS.at[top], RR.at[top], xm)
    s_r.wait_recv()
    total = PART[2, core] + SD[2].astype(F32)
    PS[low] = total[low].astype(BF16)
    KEEP[0] = total[top]
    p_b = go(PS.at[low], RL.at[low], xp)

    hf_d.wait_recv()
    s_f = mlp(3, far)
    s_f.wait_recv()
    D2S[...] = (PART[3, core] + SD[3].astype(F32)).astype(BF16)
    d_a = go(D2S.at[top], RA, xp)
    d_b = go(D2S.at[low], RB, xm)
    s_own.wait_recv()
    RES[...] = RES[...] + (PART[0, core] + SD[0].astype(F32)) + prm[5:6, :]

    d_a.wait_recv()
    PS[top] = (KEEP[0] + RA[...].astype(F32)).astype(BF16)
    p_a = go(PS.at[top], RL.at[top], xp)
    d_b.wait_recv()
    MS[low] = (KEEP[1] + RB[...].astype(F32)).astype(BF16)
    m_b = go(MS.at[low], RR.at[low], xm)

    for copy in (m_a, p_b, p_a, m_b):
        copy.wait_recv()
    out[...] = (RES[...] + RL[...].astype(F32) + RR[...].astype(F32)).astype(BF16)

    for copy in started:
        copy.wait_send()

    def sent(i, carry):
        away(0, i, 0).wait_send()
        away(0, i, 1).wait_send()
        return carry

    lax.fori_loop(1, 8, sent, 0)
    home.wait_send()
    assert len(started) <= COPIES


def local(
    tokens_in, ln1_gain, ln1_bias, qkv_weight, qkv_bias, proj_weight, proj_bias,
    ln2_gain, ln2_bias, fc1_weight, fc1_bias, fc2_weight, fc2_bias,
):
    wq = jnp.pad(qkv_weight.reshape(176, 3, HEAD), ((0, 0), (0, 0), (0, 128 - HEAD)))
    wq = wq.reshape(176, 384)
    wp = jnp.pad(proj_weight.T, ((0, 0), (0, 128 - HEAD)))
    bq = jnp.pad(qkv_bias.reshape(3, HEAD).astype(F32), ((0, 0), (0, 128 - HEAD)))
    bq = bq.at[2, HEAD].set(1.0).reshape(384)
    last = jnp.concatenate([bq, fc1_bias.astype(F32), jnp.zeros((D - 768,), F32)])
    rows = [ln1_gain, ln1_bias, proj_bias, ln2_gain, ln2_bias, fc2_bias]
    prm = jnp.stack([v.astype(F32) for v in rows] + [last, last])

    vmem = pl.BlockSpec(memory_space=pltpu.VMEM)
    hbm = pl.BlockSpec(memory_space=pl.ANY)
    dma = pltpu.SemaphoreType.DMA
    scratch = [
        pltpu.VMEM((8, 2, 128, D), BF16),
        pltpu.VMEM((4, 2, 176, 384), BF16),
        pltpu.VMEM((4, 2, 176, 2048), BF16),
        pltpu.VMEM((4, 2, 176, 768), BF16),
        pltpu.VMEM((4, 2, 176, 768), BF16),
        pltpu.VMEM((2, 8, 384), F32),
        pltpu.VMEM((8, 256, 384), BF16),
        pltpu.VMEM((8, 2, 128, 128), BF16),
        pltpu.VMEM((128, 2048), BF16),
        pltpu.VMEM((128, D), F32),
        pltpu.VMEM((4, 2, 128, D), BF16),
        pltpu.VMEM((4, 2, 128, D), F32),
        pltpu.VMEM((4, 128, D), BF16),
        pltpu.VMEM((4, 128, D), BF16),
        pltpu.VMEM((2, 64, D), F32),
        pltpu.VMEM((128, D), BF16),
        pltpu.VMEM((128, D), BF16),
        pltpu.VMEM((128, D), BF16),
        pltpu.VMEM((64, D), BF16),
        pltpu.VMEM((64, D), BF16),
        pltpu.VMEM((128, D), BF16),
        pltpu.VMEM((128, D), BF16),
        dma((COPIES,)), dma((COPIES,)), dma((16,)), dma((16,)), dma((4,)),
    ]
    return pl.pallas_call(
        kernel,
        out_shape=jax.ShapeDtypeStruct((128, D), BF16),
        in_specs=[vmem, vmem, hbm, hbm, hbm, hbm],
        out_specs=vmem,
        scratch_shapes=scratch,
        compiler_params=pltpu.CompilerParams(
            collective_id=0, has_side_effects=True, vmem_limit_bytes=62 * 1024 * 1024
        ),
    )(tokens_in, prm, wq, wp, fc1_weight, fc2_weight)


def solution(mesh):
    in_specs = (
        P(("row", "col"), None), P(), P(), P("row", "col"), P("col"), P("col", "row"), P(),
        P(), P(), P("row", "col"), P("col"), P("row", "col"), P(),
    )
    return jax.shard_map(
        local, mesh=mesh, in_specs=in_specs, out_specs=P(("row", "col"), None), check_vma=False
    )
```

```python
import jax
import jax.numpy as jnp
from jax import lax
from jax.experimental import pallas as pl
from jax.experimental.pallas import tpu as pltpu
from jax.sharding import PartitionSpec as P

MESH = pl.DeviceIdType.MESH
F32 = jnp.float32
BF16 = jnp.bfloat16
D = 1408
HEAD = 88
COPIES = 122
SENDS = 28
FR = 80
YZ, ZY = "yz", "zy"
FIRST, SECOND = ZY, YZ
PM, IO = "pm", "io"
ORDER = (
    18, 74, 54, 73, 39, 3, 40, 55, 16, 1, 2, 0, 20, 14, 41, 56, 91, 22, 27, 19, 5, 45, 17, 75, 57,
    44, 4, 89, 21, 24, 13, 23, 42, 47, 59, 15, 29, 9, 8, 6, 43, 7, 58, 28, 77, 31, 46, 25, 62, 34,
    35, 32, 30, 26, 10, 88, 11, 60, 61, 68, 12, 33, 48, 80, 67, 49, 51, 50, 64, 65, 79, 104, 71,
    103, 36, 106, 37, 98, 85, 107, 86, 97, 38, 69, 70, 105, 83, 108, 63, 109, 53, 110, 52, 113, 114,
    119, 120, 72, 95, 111, 112, 90, 123, 124, 66, 115, 116, 121, 81, 122, 117, 118, 99, 82, 94, 87,
    76, 100, 93, 101, 92, 125, 126, 127, 84, 128, 133, 139, 130, 96, 78, 136, 102, 140, 134, 131,
    145, 137, 141, 142, 132, 135, 138, 129, 148, 153, 152, 147, 144, 158, 163, 162, 150, 156, 143,
    146, 160, 173, 164, 167, 170, 149, 155, 154, 159, 165, 166, 174, 175, 168, 169, 171, 172, 151,
    157, 161, 176,
)
SLOTS = (
    0, 1, 2, 3, 4, 5, 6, 7, 8, 9, 10, 11, 12, 13, 14, 15, 16, 17, 18, 4, 2, 6, 19, 20, 21, 22, 5, 0,
    7, 8, 14, 1, 3, 10, 12, 13, 15, 2, 9, 11, 23, 24, 25, 4, 26, 21, 6, 5, 18, 7, 17, 16, 20, 3, 0,
    22, 19, 8, 14, 10, 12, 1, 13, 9, 25, 7, 11, 2, 26, 17, 27, 23, 16, 24, 6, 15, 4, 12, 21, 1, 0,
    18, 8, 19, 14, 3, 5, 10, 9, 20, 25, 16, 24, 17, 11, 13, 26, 21, 22, 23, 4, 12, 27, 2, 7, 6, 0,
    18, 15, 1, 19, 14, 8, 25, 3, 5, 10, 24, 16, 17, 20, 11, 26, 13, 9, 22, 23, 4, 21, 0, 12, 27, 7,
    18, 2, 15, 1, 6, 8, 19, 25, 14, 10, 5, 16, 11,
)
SCALE = (1.0 / HEAD**0.5) * 1.4426950408889634
NT = (((1,), (1,)), ((), ()))


def norm(values, gain, bias):
    mean = jnp.mean(values, axis=-1, keepdims=True)
    centred = values - mean
    var = jnp.mean(centred * centred, axis=-1, keepdims=True)
    return centred * lax.rsqrt(var + 1e-06) * gain + bias


class Names:
    def __getattr__(self, name):
        return name


def panel(w):
    lane = lax.broadcasted_iota(jnp.int32, (w.shape[0], 128), 1)
    rest = jnp.concatenate([w[:, 176:264], jnp.zeros((w.shape[0], 40), F32)], axis=1)
    parts = [w[:, 0:128], w[:, 88:216], rest]
    return [jnp.where(lane < HEAD, part, 0.0) for part in parts]


def kernel(
    tok_in, g1, b1, pb, g2, b2, cb, qb, fb, wq, wp, f1, f2, out,
    X, WQ, QB, WP, F1, F2, FB, QKV, O, OA, PP, PS, PR, RES, H, PART, SS, SD, KEEP, DS, RS_R, RS_L,
    RA, RB, RL, RR, tok, QR, WR, WT, v0, v1, v2, v3, v4, v5, vq, vf,
    send, recv, lsem,
):
    r = lax.axis_index("row")
    c = lax.axis_index("col")
    z, yh = r // 2, r % 2
    x, yl, core = c // 4, (c // 2) % 2, c % 2
    y = yh * 2 + yl
    chip = c // 2

    def plus(v, n):
        return lax.rem(v + n, 4)

    def at_x(v):
        return (r, v * 4 + yl * 2 + core)

    def at_y(v):
        return (z * 2 + v // 2, x * 4 + lax.rem(v, 2) * 2 + core)

    def at_z(v):
        return (v * 2 + yh, c)

    left, right, far = plus(x, 3), plus(x, 1), plus(x, 2)
    zb, zf, z2 = plus(z, 3), plus(z, 1), plus(z, 2)
    yi, yo, y2 = yh * 2 + 1 - yl, plus(y, 3 + 2 * yl), plus(y, 2)
    xs = {"p": at_x(right), "m": at_x(left)}
    ys = {"i": at_y(yi), "o": at_y(yo)}
    zs = {"p": at_z(zf), "m": at_z(zb)}
    dd = (r, x * 4 + yl * 2 + 1 - core)

    barrier = pltpu.get_barrier_semaphore()
    peers = [*xs.values(), *ys.values(), *zs.values(), dd]
    for peer in peers:
        pl.semaphore_signal(barrier, inc=1, device_id=peer, device_id_type=MESH)

    def cols(yv):
        return pl.ds(pl.multiple_of(lax.rem(yv, 2) * 384, 384), 384)

    def lanes(xv, yv):
        return pl.ds(pl.multiple_of(lax.rem(yv, 2) * 512 + xv * 128, 128), 128)

    def line(yv):
        return pl.ds(pl.multiple_of(lax.rem(yv, 2) * 512, 512), 512)

    def piece(F, zv, yv):
        return F.at[zv, yv // 2, :, cols(yv)]

    pairs = [
        (tok_in, tok), (g1, v0), (b1, v1), (wq, QR), (wp, WR), (qb, vq), (pb, v2), (g2, v3),
        (b2, v4), (cb, v5), (fb, vf), (f2, piece(F2, z, y)), (f1, piece(F1, z, y)),
    ]
    loads = [pltpu.make_async_copy(src, dst, lsem.at[i]) for i, (src, dst) in enumerate(pairs)]
    for load in loads:
        load.start()

    def row(ref):
        return ref[...].astype(F32).reshape(1, -1)

    with jax.named_scope("prep"):
        for load in loads[:11]:
            load.wait()
        inputs = tok[...].astype(F32)
        X[chip, core] = norm(inputs, row(v0), row(v1)).astype(BF16)
        for i, part in enumerate(panel(QR[...].astype(F32))):
            WQ[z, yh, :, i * 128 : (i + 1) * 128] = part.astype(BF16)
        WT[...] = jnp.zeros((128, 256), F32)
        WT[0:HEAD, 0:176] = WR[...].astype(F32)
        WP[z, yh, :, lanes(x, yl)] = WT[...].T[0:176].astype(BF16)
        FB[yl] = jnp.broadcast_to(row(vf), (8, 384))
        for load in loads[11:]:
            load.wait()
    with jax.named_scope("w_barrier"):
        pl.semaphore_wait(barrier, len(peers))

    t = Names()
    acts = {}

    def push(name, deps, ref, dev):
        acts[name] = (deps, ref, ref, dev)

    def go(name, deps, src, dst, dev):
        acts[name] = (deps, src, dst, dev)

    def calc(name, deps, step):
        acts[name] = (deps, step)

    top, low = pl.ds(0, 64), pl.ds(64, 64)
    ra, rb = pl.ds(0, 96), pl.ds(96, 80)

    def blk(xv, yv, rows=None):
        where = xv * 2 + lax.rem(yv, 2)
        return X.at[where, core] if rows is None else X.at[where, core, rows]

    push(t.qzp, [], WQ.at[z, yh], zs[t.p])
    push(t.qzm, [], WQ.at[z, yh], zs[t.m])
    go(t.qr1, [], WQ.at[z, yh, ra], QB.at[ra], ys[t.i])
    go(t.qr2, [], WQ.at[z, yh, rb], QB.at[rb], ys[t.i])
    go(t.qf1, [t.qr1], QB.at[ra], WQ.at[z, yh, ra], ys[t.o])
    go(t.qf2, [t.qr2], QB.at[rb], WQ.at[z, yh, rb], ys[t.o])
    push(t.qzfp, [t.qzp], WQ.at[zb, yh, ra], zs[t.p])
    push(t.qzfm, [t.qzm], WQ.at[zf, yh, rb], zs[t.m])
    for d in PM:
        push(t.q2z + d, [t.qf1, t.qf2], WQ.at[z, 1 - yh], zs[d])
    push(t.q2zfp, [t.q2zp], WQ.at[zb, 1 - yh, ra], zs[t.p])
    push(t.q2zfm, [t.q2zm], WQ.at[zf, 1 - yh, rb], zs[t.m])

    push(t.ad, [], blk(x, yl), dd)
    push(t.by, [], FB.at[yl], ys[t.i])
    near = {t.p: (left, top, low), t.m: (right, low, top)}
    quarter = {t.p: (t.a, pl.ds(0, 32), t.b, pl.ds(32, 32)), t.m: (t.a, pl.ds(64, 32), t.b, pl.ds(96, 32))}
    quarters = [
        (d, near[d][0], e, rows) for d, (e1, r1, e2, r2) in quarter.items() for e, rows in ((e1, r1), (e2, r2))
    ]
    for d, side, e, rows in quarters:
        push(t.a1 + e + d, [], blk(x, yl, rows), xs[d])
        push(t.af + e + d, [t.a1 + e + d], blk(side, yl, rows), xs[d])
    for d, (side, first, second) in near.items():
        push(t.a2 + d, [], blk(x, yl, second), xs[d])
    for k, rows in (("1", top), ("2", low)):
        push(t.ay + k, [], blk(x, yl, rows), ys[t.i])
        for d in PM:
            push(t.yx + k + d, [t.ay + k], blk(x, 1 - yl, rows), xs[d])
    push(t.d2y1, [t.afap, t.afbp], blk(far, yl, top), ys[t.i])
    push(t.d2y2, [t.afam, t.afbm], blk(far, yl, low), ys[t.i])
    push(t.ld, [t.a1ap, t.a1bp, t.a2p], blk(left, yl), dd)
    push(t.rd, [t.a1am, t.a1bm, t.a2m], blk(right, yl), dd)
    push(t.p0d, [t.ay1, t.ay2], blk(x, 1 - yl), dd)
    push(t.d2d, [t.afap, t.afbp, t.afam, t.afbm], blk(far, yl), dd)
    push(t.pld, [t.yx1p, t.yx2p], blk(left, 1 - yl), dd)
    push(t.prd, [t.yx1m, t.yx2m], blk(right, 1 - yl), dd)
    push(t.pd2d, [t.d2y1, t.d2y2], blk(far, 1 - yl), dd)

    ua, ub = pl.ds(0, FR), pl.ds(FR, 176 - FR)
    for d in IO:
        push(t.wa + d, [], WP.at[z, yh, ua, lanes(x, yl)], ys[d])
    push(t.waf, [t.wai], WP.at[z, yi // 2, ua, lanes(x, yi)], ys[t.o])
    waz = [t.wazfp, t.wazfm]
    for d in PM:
        for v in (0, 1):
            waz.append(t.waz + str(v) + d)
            push(waz[-1], [t.wai, t.wao, t.waf], WP.at[z, :, ua, lanes(x, v)], zs[d])
    push(t.wazfp, [t.waz0p], WP.at[zb, :, ua, lanes(x, 0)], zs[t.p])
    push(t.wazfm, [t.waz1m], WP.at[zf, :, ua, lanes(x, 1)], zs[t.m])
    whole = [t.waxfp, t.waxfm]
    for d in PM:
        for v in (0, 1):
            whole.append(t.wax + str(v) + d)
            push(whole[-1], waz, WP.at[:, :, ua, lanes(x, v)], xs[d])
    push(t.waxfp, [t.wax0p], WP.at[:, :, ua, lanes(left, 0)], xs[t.p])
    push(t.waxfm, [t.wax1m], WP.at[:, :, ua, lanes(right, 1)], xs[t.m])
    wide = (176 - FR) // 2
    push(t.wbxp, [], WP.at[z, yh, ub, lanes(x, yl)], xs[t.p])
    push(t.wbxm, [], WP.at[z, yh, ub, lanes(x, yl)], xs[t.m])
    push(t.wbxfp, [t.wbxp], WP.at[z, yh, pl.ds(FR, wide), lanes(left, yl)], xs[t.p])
    push(t.wbxfm, [t.wbxm], WP.at[z, yh, pl.ds(FR + wide, wide), lanes(right, yl)], xs[t.m])
    wbx = [t.wbxp, t.wbxm, t.wbxfp, t.wbxfm]

    def wline(zv, yv):
        return WP.at[zv, yv // 2, ub, line(yv)]

    push(t.wbyi, wbx, wline(z, y), ys[t.i])
    push(t.wbyo, wbx, wline(z, y), ys[t.o])
    push(t.wbyf, [t.wbyi], wline(z, yi), ys[t.o])
    for j, (yv, deps) in enumerate(((y, wbx), (yi, [t.wbyi]), (yo, [t.wbyo]), (y2, [t.wbyf]))):
        name = t.wbz + str(j)
        push(name + t.p, deps, wline(z, yv), zs[t.p])
        push(name + t.m, deps, wline(z, yv), zs[t.m])
        d, zv = (t.p, zb) if j < 2 else (t.m, zf)
        push(t.wbzf + str(j), [name + d], wline(zv, yv), zs[d])
        whole += [name + t.p, name + t.m, t.wbzf + str(j)]

    panels = [t.by]

    def spread(n, F, order, flip):
        if order == YZ:
            push(n + t.yi, [], piece(F, z, y), ys[t.i])
            push(n + t.yo, [], piece(F, z, y), ys[t.o])
            push(n + t.yf, [n + t.yi], piece(F, z, yi), ys[t.o])
            panels.extend([n + t.yi, n + t.yo, n + t.yf])
            parts = ((y, []), (yi, [n + t.yi]), (yo, [n + t.yo]), (y2, [n + t.yf]))
            for j, (yv, deps) in enumerate(parts):
                name = n + t.z + str(j)
                push(name + t.p, deps, piece(F, z, yv), zs[t.p])
                push(name + t.m, deps, piece(F, z, yv), zs[t.m])
                d, zv = (t.p, zb) if j < 2 else (t.m, zf)
                push(n + t.zf + str(j), [name + d], piece(F, zv, yv), zs[d])
                panels.extend([name + t.p, name + t.m, n + t.zf + str(j)])
        else:
            push(n + t.zp, [], piece(F, z, y), zs[t.p])
            push(n + t.zm, [], piece(F, z, y), zs[t.m])
            d, zv = (t.m, zf) if flip else (t.p, zb)
            push(n + t.zf, [n + t.z + d], piece(F, zv, y), zs[d])
            panels.extend([n + t.zp, n + t.zm, n + t.zf])
            parts = ((z, []), (zb, [n + t.zp]), (zf, [n + t.zm]), (z2, [n + t.zf]))
            for j, (zv, deps) in enumerate(parts):
                push(n + t.yi + str(j), deps, piece(F, zv, y), ys[t.i])
                push(n + t.yo + str(j), deps, piece(F, zv, y), ys[t.o])
                push(n + t.yf + str(j), [n + t.yi + str(j)], piece(F, zv, yi), ys[t.o])
                panels.extend([n + t.yi + str(j), n + t.yo + str(j), n + t.yf + str(j)])

    spread(t.f1, F1, FIRST, True)
    spread(t.f2, F2, SECOND, False)

    bias = jnp.concatenate(panel(row(vq)), axis=1)
    ones = lax.broadcasted_iota(jnp.int32, (1, 384), 1) == 256 + HEAD
    bias = jnp.where(ones, 1.0, bias)

    spots = [
        (x, yl), (left, yl), (right, yl), (x, 1 - yl), (far, yl),
        (left, 1 - yl), (right, 1 - yl), (far, 1 - yl),
    ]

    def qkv(j):
        def step():
            xv, yv = spots[j]
            h = X[xv * 2 + lax.rem(yv, 2)].reshape(256, D)
            product = jnp.dot(h, WQ[...].reshape(D, 384), preferred_element_type=F32)
            QKV[j] = (product + bias).astype(BF16)

        return step

    weights = [
        t.qzp, t.qzm, t.qf1, t.qf2, t.qzfp, t.qzfm, t.q2zp, t.q2zm, t.q2zfp, t.q2zfm,
    ]
    calc(t.k0, weights + [t.ad], qkv(0))
    calc(t.k1, weights + [t.ld, t.a1ap, t.a1bp, t.a2p], qkv(1))
    calc(t.k2, weights + [t.rd, t.a1am, t.a1bm, t.a2m], qkv(2))
    calc(t.k3, weights + [t.p0d, t.ay1, t.ay2], qkv(3))
    calc(t.k4, weights + [t.d2d, t.afap, t.afbp, t.afam, t.afbm], qkv(4))
    calc(t.k5, weights + [t.pld, t.yx1p, t.yx2p], qkv(5))
    calc(t.k6, weights + [t.prd, t.yx1m, t.yx2m], qkv(6))
    calc(t.k7, weights + [t.pd2d, t.d2y1, t.d2y2], qkv(7))

    slot = lanes(x, yl)

    def attend(j):
        def step():
            keys = QKV[:, :, 128:256].reshape(2048, 128)
            values = QKV[:, :, 256:384].reshape(2048, 128)

            def scores(i):
                q = QKV[j, i * 128 : i * 128 + 128, 0:128]
                return lax.dot_general(q, keys, NT, preferred_element_type=F32)

            def mix(i, s):
                most = jnp.max(s, axis=-1, keepdims=True)
                p = jnp.exp2((s - most) * SCALE).astype(BF16)
                mixed = jnp.dot(p, values, preferred_element_type=F32)
                o = (mixed / mixed[:, HEAD : HEAD + 1]).astype(BF16)
                if j == 0:
                    OA[i, :, slot] = o
                else:
                    O[j, i] = o

            first, second = scores(0), scores(1)
            mix(0, first)
            mix(1, second)

        return step

    every = [t.k + str(i) for i in range(8)]
    homes = []
    for i, j in enumerate((7, 4, 5, 1, 6, 2, 3, 0)):
        calc(t.at + str(i), every, attend(j))
        if j:
            xv, yv = spots[j]
            whose = (r, (xv * 2 + lax.rem(yv, 2)) * 2 + core)
            go(t.o + str(i), [t.at + str(i)], O.at[j], OA.at[:, :, slot], whose)
            homes.append(t.o + str(i))

    def project():
        heads = OA[...].reshape(256, 1024)
        part = lax.dot_general(heads, WP[...].reshape(D, 1024), NT, preferred_element_type=F32)
        PP[...] = part.reshape(2, 128, D)
        PS[...] = PP[1 - core].astype(BF16)

    calc(t.pr, whole + homes + [t.at + str(i) for i in range(8)], project)
    go(t.ps, [t.pr], PS, PR, dd)

    def second_norm():
        resid = tok[...].astype(F32) + PP[core] + PR[...].astype(F32) + row(v2)
        RES[...] = resid
        H[x, core] = norm(resid, row(v3), row(v4)).astype(BF16)

    calc(t.ln, [t.pr, t.ps], second_norm)

    push(t.hd, [t.ln], H.at[x, core], dd)
    for d, side, e, rows in quarters:
        push(t.h1 + e + d, [t.ln], H.at[x, core, rows], xs[d])
        push(t.hf + e + d, [t.h1 + e + d], H.at[side, core, rows], xs[d])
        other = t.m if d == t.p else t.p
        push(t.h2 + e + other, [t.ln], H.at[x, core, rows], xs[other])
    for d, (side, first, second) in near.items():
        push(t.hd1 + d, [t.h1 + t.a + d, t.h1 + t.b + d], H.at[side, core, first], dd)
        push(t.hd2 + d, [t.h2 + t.a + d, t.h2 + t.b + d], H.at[side, core, second], dd)
        push(t.hfd + d, [t.hf + t.a + d, t.hf + t.b + d], H.at[far, core, first], dd)

    def rows_of(v):
        return slice(v * 64, v * 64 + 64)

    def mlp(*parts):
        def step():
            h = [H[where, :, rows_of(v), :].reshape(128, D) for _, where, v in parts]
            h = jnp.concatenate(h, axis=0)
            a = jnp.dot(h, F1[...].reshape(D, 768), preferred_element_type=F32)
            a = a + jnp.concatenate([FB[0, 0:1, :], FB[1, 0:1, :]], axis=1)
            hidden = (0.5 * a * (1.0 + lax.erf(a * 0.7071067811865476))).astype(BF16)
            part = lax.dot_general(hidden, F2[...].reshape(D, 768), NT, preferred_element_type=F32)
            for i, (k, _, v) in enumerate(parts):
                PART[k, :, rows_of(v), :] = part[i * 128 : i * 128 + 128].reshape(2, 64, D)
                SS[k, rows_of(v), :] = PART[k, 1 - core, rows_of(v), :].astype(BF16)

        return step

    arrived_1 = [t.hd1p, t.hd1m, t.h1ap, t.h1bp, t.h1am, t.h1bm]
    arrived_2 = [t.hd2p, t.hd2m, t.h2ap, t.h2bp, t.h2am, t.h2bm]
    arrived_f = [t.hfdp, t.hfdm, t.hfap, t.hfbp, t.hfam, t.hfbm]
    calc(t.mA, panels + arrived_1, mlp((1, left, 0), (2, right, 1)))
    calc(t.mB, panels + arrived_2, mlp((1, left, 1), (2, right, 0)))
    calc(t.mF, panels + arrived_f, mlp((3, far, 0), (3, far, 1)))
    calc(t.mo, panels + [t.ln, t.hd], mlp((0, x, 0), (0, x, 1)))
    go(t.sAp, [t.mA], SS.at[1, top], SD.at[1, top], dd)
    go(t.sAm, [t.mA], SS.at[2, low], SD.at[2, low], dd)
    go(t.sBp, [t.mB], SS.at[1, low], SD.at[1, low], dd)
    go(t.sBm, [t.mB], SS.at[2, top], SD.at[2, top], dd)
    go(t.sF, [t.mF], SS.at[3], SD.at[3], dd)
    go(t.so, [t.mo], SS.at[0], SD.at[0], dd)

    def total(k, v=None):
        rows = slice(0, 128) if v is None else rows_of(v)
        return PART[k, core, rows, :] + SD[k, rows, :].astype(F32)

    def sum_first():
        RS_L[0:64] = total(1, 0).astype(BF16)
        RS_R[64:128] = total(2, 1).astype(BF16)

    def sum_second():
        KEEP[1] = total(1, 1)
        KEEP[0] = total(2, 0)

    def sum_far():
        DS[...] = total(3).astype(BF16)

    def sum_own():
        RES[...] = RES[...] + total(0) + row(v5)

    def add(mine, kept, came, lo):
        def step():
            rows = slice(lo % 64, lo % 64 + 32)
            mine[lo : lo + 32] = (KEEP[kept, rows, :] + came[rows].astype(F32)).astype(BF16)

        return step

    def finish():
        out[...] = (RES[...] + RL[...].astype(F32) + RR[...].astype(F32)).astype(BF16)

    calc(t.cA, [t.mA, t.sAp, t.sAm], sum_first)
    calc(t.cB, [t.mB, t.sBp, t.sBm], sum_second)
    calc(t.cF, [t.mF, t.sF], sum_far)
    calc(t.co, [t.mo, t.so, t.ln], sum_own)
    go(t.ma, [t.cA], RS_L.at[top], RR.at[top], xs[t.m])
    go(t.pb, [t.cA], RS_R.at[low], RL.at[low], xs[t.p])
    last = [t.co, t.ma, t.pb]
    for d, side, e, rows in quarters:
        lo = (0 if d == t.p else 64) + (0 if e == t.a else 32)
        came, mine, kept, dest = (RA, RS_R, 0, RL) if d == t.p else (RB, RS_L, 1, RR)
        go(t.da + e + d, [t.cF], DS.at[rows], came.at[pl.ds(lo % 64, 32)], xs[d])
        calc(t.e + e + d, [t.cB, t.da + e + d], add(mine, kept, came, lo))
        go(t.p + e + d, [t.e + e + d], mine.at[rows], dest.at[rows], xs[d])
        last.append(t.p + e + d)
    calc(t.end, last, finish)

    names = list(acts)
    moves = [name for name in names if len(acts[name]) == 4]
    passed_on = {dep for name in moves for dep in acts[name][0]}

    def finals(prefix):
        return [name for name in moves if name.startswith(prefix) and name not in passed_on]

    groups = [
        (homes, O.at[pl.ds(1, 7)]),
        (finals(t.f1), F1.at[pl.ds(0, 2)]),
        (finals(t.f2), F2.at[pl.ds(0, 2)]),
        (finals(t.wbz), WP.at[pl.ds(0, 2), :, ub, :]),
        (finals(t.wax), WP.at[:, :, ua, pl.ds(0, 512)]),
    ]
    assert [len(members) for members, _ in groups] == [7, 8, 8, 8, 4]
    group_of = {name: g for g, (members, _) in enumerate(groups) for name in members}
    early = [name for name in moves if name[0] in t.aq or name in (t.ld, t.rd, t.p0d, t.pld, t.prd)]
    early += [name for name in moves if name[:2] == t.yx or name[:2] == t.d2 or name == t.pd2d]
    late = moves[moves.index(t.hd):]
    slots = {name: i for i, name in enumerate(early)}
    slots.update(zip(late, range(len(late))))
    count = len(early)
    for name in moves:
        if name not in slots:
            if name in group_of:
                for member in groups[group_of[name]][0]:
                    slots[member] = count
            else:
                slots[name] = count
            count += 1
    assert len(early) >= len(late) and count <= COPIES

    done, sent, arrived, busy = set(), {}, set(), {}

    def expect(dep):
        if dep in arrived:
            return
        with jax.named_scope("w_" + dep):
            if dep in group_of:
                members, ref = groups[group_of[dep]]
                pltpu.make_async_remote_copy(
                    src_ref=ref, dst_ref=ref, send_sem=send.at[0], recv_sem=recv.at[slots[dep]],
                    device_id=dd, device_id_type=MESH,
                ).wait_recv()
                arrived.update(members)
            else:
                sent[dep].wait_recv()
                arrived.add(dep)

    turn = 0
    for number in ORDER:
        name = names[number]
        deps = acts[name][0]
        for dep in deps:
            assert dep in done
            if dep in sent:
                expect(dep)
        if len(acts[name]) == 2:
            with jax.named_scope("c_" + name):
                acts[name][1]()
        else:
            _, src, dst, dev = acts[name]
            i = SLOTS[turn]
            turn += 1
            if i in busy:
                with jax.named_scope("s_" + busy[i]):
                    sent[busy[i]].wait_send()
            busy[i] = name
            sent[name] = pltpu.make_async_remote_copy(
                src_ref=src, dst_ref=dst, send_sem=send.at[i], recv_sem=recv.at[slots[name]],
                device_id=dev, device_id_type=MESH,
            )
            sent[name].start()
        done.add(name)
    assert len(done) == len(acts)
    for name in moves:
        expect(name)
    for name in busy.values():
        sent[name].wait_send()


def local(
    tokens_in, ln1_gain, ln1_bias, qkv_weight, qkv_bias, proj_weight, proj_bias,
    ln2_gain, ln2_bias, fc1_weight, fc1_bias, fc2_weight, fc2_bias,
):
    vmem = pl.BlockSpec(memory_space=pltpu.VMEM)
    hbm = pl.BlockSpec(memory_space=pltpu.HBM)
    dma = pltpu.SemaphoreType.DMA
    def big(*shape):
        return pltpu.VMEM(shape, BF16)

    scratch = [
        big(8, 2, 128, D), big(4, 2, 176, 384), big(176, 384), big(4, 2, 176, 1024),
        big(4, 2, 176, 768), big(4, 2, 176, 768), pltpu.VMEM((2, 8, 384), F32),
        big(8, 256, 384), big(8, 2, 128, 128), big(2, 128, 1024), pltpu.VMEM((2, 128, D), F32),

        big(128, D), big(128, D), pltpu.VMEM((128, D), F32), big(4, 2, 128, D),
        pltpu.VMEM((4, 2, 128, D), F32), big(4, 128, D), big(4, 128, D), pltpu.VMEM((2, 64, D), F32),
        big(128, D), big(128, D), big(128, D), big(64, D), big(64, D), big(128, D), big(128, D),
        big(128, D), big(176, 264), big(HEAD, 176), pltpu.VMEM((128, 256), F32),
        *[big(n) for n in (D, D, D, D, D, D, 264, 384)],
        dma((SENDS,)), dma((COPIES,)), dma((13,)),
    ]
    return pl.pallas_call(
        kernel,
        out_shape=pltpu.VMEM((128, D), BF16),
        in_specs=[hbm] * 13,
        out_specs=vmem,
        scratch_shapes=scratch,
        compiler_params=pltpu.CompilerParams(
            collective_id=0, has_side_effects=True, vmem_limit_bytes=62 * 1024 * 1024
        ),
    )(
        tokens_in, ln1_gain, ln1_bias, proj_bias, ln2_gain, ln2_bias, fc2_bias, qkv_bias, fc1_bias,
        qkv_weight, proj_weight, fc1_weight, fc2_weight,
    )


def solution(mesh):
    in_specs = (
        P(("row", "col"), None), P(), P(), P("row", "col"), P("col"), P("col", "row"), P(),
        P(), P(), P("row", "col"), P("col"), P("row", "col"), P(),
    )
    return jax.shard_map(
        local, mesh=mesh, in_specs=in_specs, out_specs=P(("row", "col"), None), check_vma=False
    )
```

```python
import jax
import jax.numpy as jnp
from jax import lax
from jax.experimental import pallas as pl
from jax.experimental.pallas import tpu as pltpu
from jax.sharding import PartitionSpec as P

MESH = pl.DeviceIdType.MESH
F32 = jnp.float32
BF16 = jnp.bfloat16
D = 1408
HEAD = 88
COPIES = 122
SENDS = 28
FR = 80
YZ, ZY = "yz", "zy"
FIRST, SECOND = ZY, YZ
PM, IO = "pm", "io"
ORDER = (
    18, 74, 54, 73, 39, 3, 40, 55, 16, 1, 2, 0, 20, 14, 41, 56, 91, 22, 27, 19, 5, 45, 17, 75, 57,
    44, 4, 89, 21, 24, 13, 23, 42, 47, 59, 15, 29, 9, 8, 6, 43, 7, 58, 28, 77, 31, 46, 25, 62, 34,
    35, 32, 30, 26, 10, 88, 11, 60, 61, 68, 12, 33, 48, 80, 67, 49, 51, 50, 64, 65, 79, 104, 71,
    103, 36, 106, 37, 98, 85, 107, 86, 97, 38, 69, 70, 105, 83, 108, 63, 109, 53, 110, 52, 113, 114,
    119, 120, 72, 95, 111, 112, 90, 123, 124, 66, 115, 116, 121, 81, 122, 117, 118, 99, 82, 94, 87,
    76, 100, 93, 101, 92, 125, 126, 127, 84, 128, 130, 136, 133, 139, 129, 96, 78, 102, 131, 137,
    134, 140, 145, 141, 142, 132, 135, 138, 148, 153, 152, 147, 144, 158, 163, 162, 150, 156, 143,
    146, 160, 173, 164, 167, 170, 149, 155, 154, 159, 165, 166, 174, 175, 168, 169, 171, 172, 151,
    157, 161, 176,
)
SLOTS = (
    0, 1, 2, 3, 4, 5, 6, 7, 8, 9, 10, 11, 12, 13, 14, 15, 16, 17, 18, 4, 2, 6, 19, 20, 21, 22, 5, 0,
    7, 8, 14, 1, 3, 10, 12, 13, 15, 2, 9, 11, 23, 24, 25, 4, 26, 21, 6, 5, 18, 7, 17, 16, 20, 3, 0,
    22, 19, 8, 14, 10, 12, 1, 13, 9, 25, 7, 11, 2, 26, 17, 27, 23, 16, 24, 6, 15, 4, 12, 21, 1, 0,
    18, 8, 19, 14, 3, 5, 10, 9, 20, 25, 16, 24, 17, 11, 13, 26, 21, 22, 23, 4, 12, 27, 2, 7, 6, 0,
    18, 15, 1, 19, 14, 8, 25, 3, 5, 10, 24, 16, 17, 20, 11, 26, 13, 9, 22, 23, 4, 21, 0, 12, 27, 8,
    7, 18, 2, 15, 1, 6, 3, 19, 14, 25, 10, 24, 20,
)
SCALE = (1.0 / HEAD**0.5) * 1.4426950408889634
NT = (((1,), (1,)), ((), ()))


def norm(values, gain, bias):
    mean = jnp.mean(values, axis=-1, keepdims=True)
    centred = values - mean
    var = jnp.mean(centred * centred, axis=-1, keepdims=True)
    return centred * lax.rsqrt(var + 1e-06) * gain + bias


class Names:
    def __getattr__(self, name):
        return name


def panel(w):
    lane = lax.broadcasted_iota(jnp.int32, (w.shape[0], 128), 1)
    rest = jnp.concatenate([w[:, 176:264], jnp.zeros((w.shape[0], 40), F32)], axis=1)
    parts = [w[:, 0:128], w[:, 88:216], rest]
    return [jnp.where(lane < HEAD, part, 0.0) for part in parts]


def kernel(
    tok_in, g1, b1, pb, g2, b2, cb, qb, fb, wq, wp, f1, f2, out,
    X, WQ, QB, WP, F1, F2, FB, QKV, O, OA, PP, PS, PR, RES, H, PART, SS, SD, KEEP, DS, RS_R, RS_L,
    RA, RB, RL, RR, tok, QR, WR, WT, v0, v1, v2, v3, v4, v5, vq, vf,
    send, recv, lsem,
):
    r = lax.axis_index("row")
    c = lax.axis_index("col")
    z, yh = r // 2, r % 2
    x, yl, core = c // 4, (c // 2) % 2, c % 2
    y = yh * 2 + yl
    chip = c // 2

    def plus(v, n):
        return lax.rem(v + n, 4)

    def at_x(v):
        return (r, v * 4 + yl * 2 + core)

    def at_y(v):
        return (z * 2 + v // 2, x * 4 + lax.rem(v, 2) * 2 + core)

    def at_z(v):
        return (v * 2 + yh, c)

    left, right, far = plus(x, 3), plus(x, 1), plus(x, 2)
    zb, zf, z2 = plus(z, 3), plus(z, 1), plus(z, 2)
    yi, yo, y2 = yh * 2 + 1 - yl, plus(y, 3 + 2 * yl), plus(y, 2)
    xs = {"p": at_x(right), "m": at_x(left)}
    ys = {"i": at_y(yi), "o": at_y(yo)}
    zs = {"p": at_z(zf), "m": at_z(zb)}
    dd = (r, x * 4 + yl * 2 + 1 - core)

    barrier = pltpu.get_barrier_semaphore()
    peers = [*xs.values(), *ys.values(), *zs.values(), dd]
    for peer in peers:
        pl.semaphore_signal(barrier, inc=1, device_id=peer, device_id_type=MESH)

    def cols(yv):
        return pl.ds(pl.multiple_of(lax.rem(yv, 2) * 384, 384), 384)

    def lanes(xv, yv):
        return pl.ds(pl.multiple_of(lax.rem(yv, 2) * 512 + xv * 128, 128), 128)

    def line(yv):
        return pl.ds(pl.multiple_of(lax.rem(yv, 2) * 512, 512), 512)

    def piece(F, zv, yv):
        return F.at[zv, yv // 2, :, cols(yv)]

    pairs = [
        (tok_in, tok), (g1, v0), (b1, v1), (wq, QR), (wp, WR), (qb, vq), (pb, v2), (g2, v3),
        (b2, v4), (cb, v5), (fb, vf), (f2, piece(F2, z, y)), (f1, piece(F1, z, y)),
    ]
    loads = [pltpu.make_async_copy(src, dst, lsem.at[i]) for i, (src, dst) in enumerate(pairs)]
    for load in loads:
        load.start()

    def row(ref):
        return ref[...].astype(F32).reshape(1, -1)

    with jax.named_scope("prep"):
        for load in loads[:11]:
            load.wait()
        inputs = tok[...].astype(F32)
        X[chip, core] = norm(inputs, row(v0), row(v1)).astype(BF16)
        for i, part in enumerate(panel(QR[...].astype(F32))):
            WQ[z, yh, :, i * 128 : (i + 1) * 128] = part.astype(BF16)
        WT[...] = jnp.zeros((128, 256), F32)
        WT[0:HEAD, 0:176] = WR[...].astype(F32)
        WP[z, yh, :, lanes(x, yl)] = WT[...].T[0:176].astype(BF16)
        FB[yl] = jnp.broadcast_to(row(vf), (8, 384))
        for load in loads[11:]:
            load.wait()
    with jax.named_scope("w_barrier"):
        pl.semaphore_wait(barrier, len(peers))

    t = Names()
    acts = {}

    def push(name, deps, ref, dev):
        acts[name] = (deps, ref, ref, dev)

    def go(name, deps, src, dst, dev):
        acts[name] = (deps, src, dst, dev)

    def calc(name, deps, step):
        acts[name] = (deps, step)

    top, low = pl.ds(0, 64), pl.ds(64, 64)
    ra, rb = pl.ds(0, 96), pl.ds(96, 80)

    def blk(xv, yv, rows=None):
        where = xv * 2 + lax.rem(yv, 2)
        return X.at[where, core] if rows is None else X.at[where, core, rows]

    push(t.qzp, [], WQ.at[z, yh], zs[t.p])
    push(t.qzm, [], WQ.at[z, yh], zs[t.m])
    go(t.qr1, [], WQ.at[z, yh, ra], QB.at[ra], ys[t.i])
    go(t.qr2, [], WQ.at[z, yh, rb], QB.at[rb], ys[t.i])
    go(t.qf1, [t.qr1], QB.at[ra], WQ.at[z, yh, ra], ys[t.o])
    go(t.qf2, [t.qr2], QB.at[rb], WQ.at[z, yh, rb], ys[t.o])
    push(t.qzfp, [t.qzp], WQ.at[zb, yh, ra], zs[t.p])
    push(t.qzfm, [t.qzm], WQ.at[zf, yh, rb], zs[t.m])
    for d in PM:
        push(t.q2z + d, [t.qf1, t.qf2], WQ.at[z, 1 - yh], zs[d])
    push(t.q2zfp, [t.q2zp], WQ.at[zb, 1 - yh, ra], zs[t.p])
    push(t.q2zfm, [t.q2zm], WQ.at[zf, 1 - yh, rb], zs[t.m])

    push(t.ad, [], blk(x, yl), dd)
    push(t.by, [], FB.at[yl], ys[t.i])
    near = {t.p: (left, top, low), t.m: (right, low, top)}
    quarter = {t.p: (t.a, pl.ds(0, 32), t.b, pl.ds(32, 32)), t.m: (t.a, pl.ds(64, 32), t.b, pl.ds(96, 32))}
    quarters = [
        (d, near[d][0], e, rows) for d, (e1, r1, e2, r2) in quarter.items() for e, rows in ((e1, r1), (e2, r2))
    ]
    for d, side, e, rows in quarters:
        push(t.a1 + e + d, [], blk(x, yl, rows), xs[d])
        push(t.af + e + d, [t.a1 + e + d], blk(side, yl, rows), xs[d])
    for d, (side, first, second) in near.items():
        push(t.a2 + d, [], blk(x, yl, second), xs[d])
    for k, rows in (("1", top), ("2", low)):
        push(t.ay + k, [], blk(x, yl, rows), ys[t.i])
        for d in PM:
            push(t.yx + k + d, [t.ay + k], blk(x, 1 - yl, rows), xs[d])
    push(t.d2y1, [t.afap, t.afbp], blk(far, yl, top), ys[t.i])
    push(t.d2y2, [t.afam, t.afbm], blk(far, yl, low), ys[t.i])
    push(t.ld, [t.a1ap, t.a1bp, t.a2p], blk(left, yl), dd)
    push(t.rd, [t.a1am, t.a1bm, t.a2m], blk(right, yl), dd)
    push(t.p0d, [t.ay1, t.ay2], blk(x, 1 - yl), dd)
    push(t.d2d, [t.afap, t.afbp, t.afam, t.afbm], blk(far, yl), dd)
    push(t.pld, [t.yx1p, t.yx2p], blk(left, 1 - yl), dd)
    push(t.prd, [t.yx1m, t.yx2m], blk(right, 1 - yl), dd)
    push(t.pd2d, [t.d2y1, t.d2y2], blk(far, 1 - yl), dd)

    ua, ub = pl.ds(0, FR), pl.ds(FR, 176 - FR)
    for d in IO:
        push(t.wa + d, [], WP.at[z, yh, ua, lanes(x, yl)], ys[d])
    push(t.waf, [t.wai], WP.at[z, yi // 2, ua, lanes(x, yi)], ys[t.o])
    waz = [t.wazfp, t.wazfm]
    for d in PM:
        for v in (0, 1):
            waz.append(t.waz + str(v) + d)
            push(waz[-1], [t.wai, t.wao, t.waf], WP.at[z, :, ua, lanes(x, v)], zs[d])
    push(t.wazfp, [t.waz0p], WP.at[zb, :, ua, lanes(x, 0)], zs[t.p])
    push(t.wazfm, [t.waz1m], WP.at[zf, :, ua, lanes(x, 1)], zs[t.m])
    whole = [t.waxfp, t.waxfm]
    for d in PM:
        for v in (0, 1):
            whole.append(t.wax + str(v) + d)
            push(whole[-1], waz, WP.at[:, :, ua, lanes(x, v)], xs[d])
    push(t.waxfp, [t.wax0p], WP.at[:, :, ua, lanes(left, 0)], xs[t.p])
    push(t.waxfm, [t.wax1m], WP.at[:, :, ua, lanes(right, 1)], xs[t.m])
    wide = (176 - FR) // 2
    push(t.wbxp, [], WP.at[z, yh, ub, lanes(x, yl)], xs[t.p])
    push(t.wbxm, [], WP.at[z, yh, ub, lanes(x, yl)], xs[t.m])
    push(t.wbxfp, [t.wbxp], WP.at[z, yh, pl.ds(FR, wide), lanes(left, yl)], xs[t.p])
    push(t.wbxfm, [t.wbxm], WP.at[z, yh, pl.ds(FR + wide, wide), lanes(right, yl)], xs[t.m])
    wbx = [t.wbxp, t.wbxm, t.wbxfp, t.wbxfm]

    def wline(zv, yv):
        return WP.at[zv, yv // 2, ub, line(yv)]

    push(t.wbyi, wbx, wline(z, y), ys[t.i])
    push(t.wbyo, wbx, wline(z, y), ys[t.o])
    push(t.wbyf, [t.wbyi], wline(z, yi), ys[t.o])
    for j, (yv, deps) in enumerate(((y, wbx), (yi, [t.wbyi]), (yo, [t.wbyo]), (y2, [t.wbyf]))):
        name = t.wbz + str(j)
        push(name + t.p, deps, wline(z, yv), zs[t.p])
        push(name + t.m, deps, wline(z, yv), zs[t.m])
        d, zv = (t.p, zb) if j < 2 else (t.m, zf)
        push(t.wbzf + str(j), [name + d], wline(zv, yv), zs[d])
        whole += [name + t.p, name + t.m, t.wbzf + str(j)]

    panels = [t.by]

    def spread(n, F, order, flip):
        if order == YZ:
            push(n + t.yi, [], piece(F, z, y), ys[t.i])
            push(n + t.yo, [], piece(F, z, y), ys[t.o])
            push(n + t.yf, [n + t.yi], piece(F, z, yi), ys[t.o])
            panels.extend([n + t.yi, n + t.yo, n + t.yf])
            parts = ((y, []), (yi, [n + t.yi]), (yo, [n + t.yo]), (y2, [n + t.yf]))
            for j, (yv, deps) in enumerate(parts):
                name = n + t.z + str(j)
                push(name + t.p, deps, piece(F, z, yv), zs[t.p])
                push(name + t.m, deps, piece(F, z, yv), zs[t.m])
                d, zv = (t.p, zb) if j < 2 else (t.m, zf)
                push(n + t.zf + str(j), [name + d], piece(F, zv, yv), zs[d])
                panels.extend([name + t.p, name + t.m, n + t.zf + str(j)])
        else:
            push(n + t.zp, [], piece(F, z, y), zs[t.p])
            push(n + t.zm, [], piece(F, z, y), zs[t.m])
            d, zv = (t.m, zf) if flip else (t.p, zb)
            push(n + t.zf, [n + t.z + d], piece(F, zv, y), zs[d])
            panels.extend([n + t.zp, n + t.zm, n + t.zf])
            parts = ((z, []), (zb, [n + t.zp]), (zf, [n + t.zm]), (z2, [n + t.zf]))
            for j, (zv, deps) in enumerate(parts):
                push(n + t.yi + str(j), deps, piece(F, zv, y), ys[t.i])
                push(n + t.yo + str(j), deps, piece(F, zv, y), ys[t.o])
                push(n + t.yf + str(j), [n + t.yi + str(j)], piece(F, zv, yi), ys[t.o])
                panels.extend([n + t.yi + str(j), n + t.yo + str(j), n + t.yf + str(j)])

    spread(t.f1, F1, FIRST, True)
    spread(t.f2, F2, SECOND, False)

    bias = jnp.concatenate(panel(row(vq)), axis=1)
    ones = lax.broadcasted_iota(jnp.int32, (1, 384), 1) == 256 + HEAD
    bias = jnp.where(ones, 1.0, bias)

    spots = [
        (x, yl), (left, yl), (right, yl), (x, 1 - yl), (far, yl),
        (left, 1 - yl), (right, 1 - yl), (far, 1 - yl),
    ]

    def qkv(j):
        def step():
            xv, yv = spots[j]
            h = X[xv * 2 + lax.rem(yv, 2)].reshape(256, D)
            product = jnp.dot(h, WQ[...].reshape(D, 384), preferred_element_type=F32)
            QKV[j] = (product + bias).astype(BF16)

        return step

    weights = [
        t.qzp, t.qzm, t.qf1, t.qf2, t.qzfp, t.qzfm, t.q2zp, t.q2zm, t.q2zfp, t.q2zfm,
    ]
    calc(t.k0, weights + [t.ad], qkv(0))
    calc(t.k1, weights + [t.ld, t.a1ap, t.a1bp, t.a2p], qkv(1))
    calc(t.k2, weights + [t.rd, t.a1am, t.a1bm, t.a2m], qkv(2))
    calc(t.k3, weights + [t.p0d, t.ay1, t.ay2], qkv(3))
    calc(t.k4, weights + [t.d2d, t.afap, t.afbp, t.afam, t.afbm], qkv(4))
    calc(t.k5, weights + [t.pld, t.yx1p, t.yx2p], qkv(5))
    calc(t.k6, weights + [t.prd, t.yx1m, t.yx2m], qkv(6))
    calc(t.k7, weights + [t.pd2d, t.d2y1, t.d2y2], qkv(7))

    slot = lanes(x, yl)

    def attend(j):
        def step():
            keys = QKV[:, :, 128:256].reshape(2048, 128)
            values = QKV[:, :, 256:384].reshape(2048, 128)

            def scores(i):
                q = QKV[j, i * 128 : i * 128 + 128, 0:128]
                return lax.dot_general(q, keys, NT, preferred_element_type=F32)

            def mix(i, s):
                most = jnp.max(s, axis=-1, keepdims=True)
                p = jnp.exp2((s - most) * SCALE).astype(BF16)
                mixed = jnp.dot(p, values, preferred_element_type=F32)
                o = (mixed / mixed[:, HEAD : HEAD + 1]).astype(BF16)
                if j == 0:
                    OA[i, :, slot] = o
                else:
                    O[j, i] = o

            first, second = scores(0), scores(1)
            mix(0, first)
            mix(1, second)

        return step

    every = [t.k + str(i) for i in range(8)]
    homes = []
    for i, j in enumerate((7, 4, 5, 1, 6, 2, 3, 0)):
        calc(t.at + str(i), every, attend(j))
        if j:
            xv, yv = spots[j]
            whose = (r, (xv * 2 + lax.rem(yv, 2)) * 2 + core)
            go(t.o + str(i), [t.at + str(i)], O.at[j], OA.at[:, :, slot], whose)
            homes.append(t.o + str(i))

    def project():
        heads = OA[...].reshape(256, 1024)
        part = lax.dot_general(heads, WP[...].reshape(D, 1024), NT, preferred_element_type=F32)
        PP[...] = part.reshape(2, 128, D)
        PS[...] = PP[1 - core].astype(BF16)

    calc(t.pr, whole + homes + [t.at + str(i) for i in range(8)], project)
    go(t.ps, [t.pr], PS, PR, dd)

    def second_norm():
        resid = tok[...].astype(F32) + PP[core] + PR[...].astype(F32) + row(v2)
        RES[...] = resid
        H[x, core] = norm(resid, row(v3), row(v4)).astype(BF16)

    calc(t.ln, [t.pr, t.ps], second_norm)

    push(t.hd, [t.ln], H.at[x, core], dd)
    for d, side, e, rows in quarters:
        push(t.h1 + e + d, [t.ln], H.at[x, core, rows], xs[d])
        push(t.hf + e + d, [t.h1 + e + d], H.at[side, core, rows], xs[d])
        other = t.m if d == t.p else t.p
        push(t.h2 + e + other, [t.ln], H.at[x, core, rows], xs[other])
    for d, (side, first, second) in near.items():
        push(t.hd1 + d, [t.h1 + t.a + d, t.h1 + t.b + d], H.at[side, core, first], dd)
        push(t.hd2 + d, [t.h2 + t.a + d, t.h2 + t.b + d], H.at[side, core, second], dd)
        push(t.hfd + d, [t.hf + t.a + d, t.hf + t.b + d], H.at[far, core, first], dd)

    def rows_of(v):
        return slice(v * 64, v * 64 + 64)

    def mlp(*parts):
        def step():
            h = [H[where, :, rows_of(v), :].reshape(128, D) for _, where, v in parts]
            h = jnp.concatenate(h, axis=0)
            a = jnp.dot(h, F1[...].reshape(D, 768), preferred_element_type=F32)
            a = a + jnp.concatenate([FB[0, 0:1, :], FB[1, 0:1, :]], axis=1)
            hidden = (0.5 * a * (1.0 + lax.erf(a * 0.7071067811865476))).astype(BF16)
            part = lax.dot_general(hidden, F2[...].reshape(D, 768), NT, preferred_element_type=F32)
            for i, (k, _, v) in enumerate(parts):
                PART[k, :, rows_of(v), :] = part[i * 128 : i * 128 + 128].reshape(2, 64, D)
                SS[k, rows_of(v), :] = PART[k, 1 - core, rows_of(v), :].astype(BF16)

        return step

    arrived_1 = [t.hd1p, t.hd1m, t.h1ap, t.h1bp, t.h1am, t.h1bm]
    arrived_2 = [t.hd2p, t.hd2m, t.h2ap, t.h2bp, t.h2am, t.h2bm]
    arrived_f = [t.hfdp, t.hfdm, t.hfap, t.hfbp, t.hfam, t.hfbm]
    calc(t.mA, panels + arrived_1, mlp((1, left, 0), (2, right, 1)))
    calc(t.mB, panels + arrived_2, mlp((1, left, 1), (2, right, 0)))
    calc(t.mF, panels + arrived_f, mlp((3, far, 0), (3, far, 1)))
    calc(t.mo, panels + [t.ln, t.hd], mlp((0, x, 0), (0, x, 1)))
    go(t.sAp, [t.mA], SS.at[1, top], SD.at[1, top], dd)
    go(t.sAm, [t.mA], SS.at[2, low], SD.at[2, low], dd)
    go(t.sBp, [t.mB], SS.at[1, low], SD.at[1, low], dd)
    go(t.sBm, [t.mB], SS.at[2, top], SD.at[2, top], dd)
    go(t.sF, [t.mF], SS.at[3], SD.at[3], dd)
    go(t.so, [t.mo], SS.at[0], SD.at[0], dd)

    def total(k, v=None):
        rows = slice(0, 128) if v is None else rows_of(v)
        return PART[k, core, rows, :] + SD[k, rows, :].astype(F32)

    def sum_first():
        RS_L[0:64] = total(1, 0).astype(BF16)
        RS_R[64:128] = total(2, 1).astype(BF16)

    def sum_second():
        KEEP[1] = total(1, 1)
        KEEP[0] = total(2, 0)

    def sum_far():
        DS[...] = total(3).astype(BF16)

    def sum_own():
        RES[...] = RES[...] + total(0) + row(v5)

    def add(mine, kept, came, lo):
        def step():
            rows = slice(lo % 64, lo % 64 + 32)
            mine[lo : lo + 32] = (KEEP[kept, rows, :] + came[rows].astype(F32)).astype(BF16)

        return step

    def finish():
        out[...] = (RES[...] + RL[...].astype(F32) + RR[...].astype(F32)).astype(BF16)

    calc(t.cA, [t.mA, t.sAp, t.sAm], sum_first)
    calc(t.cB, [t.mB, t.sBp, t.sBm], sum_second)
    calc(t.cF, [t.mF, t.sF], sum_far)
    calc(t.co, [t.mo, t.so, t.ln], sum_own)
    go(t.ma, [t.cA], RS_L.at[top], RR.at[top], xs[t.m])
    go(t.pb, [t.cA], RS_R.at[low], RL.at[low], xs[t.p])
    last = [t.co, t.ma, t.pb]
    for d, side, e, rows in quarters:
        lo = (0 if d == t.p else 64) + (0 if e == t.a else 32)
        came, mine, kept, dest = (RA, RS_R, 0, RL) if d == t.p else (RB, RS_L, 1, RR)
        go(t.da + e + d, [t.cF], DS.at[rows], came.at[pl.ds(lo % 64, 32)], xs[d])
        calc(t.e + e + d, [t.cB, t.da + e + d], add(mine, kept, came, lo))
        go(t.p + e + d, [t.e + e + d], mine.at[rows], dest.at[rows], xs[d])
        last.append(t.p + e + d)
    calc(t.end, last, finish)

    names = list(acts)
    moves = [name for name in names if len(acts[name]) == 4]
    passed_on = {dep for name in moves for dep in acts[name][0]}

    def finals(prefix):
        return [name for name in moves if name.startswith(prefix) and name not in passed_on]

    groups = [
        (homes, O.at[pl.ds(1, 7)]),
        (finals(t.f1), F1.at[pl.ds(0, 2)]),
        (finals(t.f2), F2.at[pl.ds(0, 2)]),
        (finals(t.wbz), WP.at[pl.ds(0, 2), :, ub, :]),
        (finals(t.wax), WP.at[:, :, ua, pl.ds(0, 512)]),
    ]
    assert [len(members) for members, _ in groups] == [7, 8, 8, 8, 4]
    group_of = {name: g for g, (members, _) in enumerate(groups) for name in members}
    early = [name for name in moves if name[0] in t.aq or name in (t.ld, t.rd, t.p0d, t.pld, t.prd)]
    early += [name for name in moves if name[:2] == t.yx or name[:2] == t.d2 or name == t.pd2d]
    late = moves[moves.index(t.hd):]
    slots = {name: i for i, name in enumerate(early)}
    slots.update(zip(late, range(len(late))))
    count = len(early)
    for name in moves:
        if name not in slots:
            if name in group_of:
                for member in groups[group_of[name]][0]:
                    slots[member] = count
            else:
                slots[name] = count
            count += 1
    assert len(early) >= len(late) and count <= COPIES

    done, sent, arrived, busy = set(), {}, set(), {}

    def expect(dep):
        if dep in arrived:
            return
        with jax.named_scope("w_" + dep):
            if dep in group_of:
                members, ref = groups[group_of[dep]]
                pltpu.make_async_remote_copy(
                    src_ref=ref, dst_ref=ref, send_sem=send.at[0], recv_sem=recv.at[slots[dep]],
                    device_id=dd, device_id_type=MESH,
                ).wait_recv()
                arrived.update(members)
            else:
                sent[dep].wait_recv()
                arrived.add(dep)

    turn = 0
    for number in ORDER:
        name = names[number]
        deps = acts[name][0]
        for dep in deps:
            assert dep in done
            if dep in sent:
                expect(dep)
        if len(acts[name]) == 2:
            with jax.named_scope("c_" + name):
                acts[name][1]()
        else:
            _, src, dst, dev = acts[name]
            i = SLOTS[turn]
            turn += 1
            if i in busy:
                with jax.named_scope("s_" + busy[i]):
                    sent[busy[i]].wait_send()
            busy[i] = name
            sent[name] = pltpu.make_async_remote_copy(
                src_ref=src, dst_ref=dst, send_sem=send.at[i], recv_sem=recv.at[slots[name]],
                device_id=dev, device_id_type=MESH,
            )
            sent[name].start()
        done.add(name)
    assert len(done) == len(acts)
    for name in moves:
        expect(name)
    for name in busy.values():
        sent[name].wait_send()


def local(
    tokens_in, ln1_gain, ln1_bias, qkv_weight, qkv_bias, proj_weight, proj_bias,
    ln2_gain, ln2_bias, fc1_weight, fc1_bias, fc2_weight, fc2_bias,
):
    vmem = pl.BlockSpec(memory_space=pltpu.VMEM)
    hbm = pl.BlockSpec(memory_space=pltpu.HBM)
    dma = pltpu.SemaphoreType.DMA
    def big(*shape):
        return pltpu.VMEM(shape, BF16)

    scratch = [
        big(8, 2, 128, D), big(4, 2, 176, 384), big(176, 384), big(4, 2, 176, 1024),
        big(4, 2, 176, 768), big(4, 2, 176, 768), pltpu.VMEM((2, 8, 384), F32),
        big(8, 256, 384), big(8, 2, 128, 128), big(2, 128, 1024), pltpu.VMEM((2, 128, D), F32),

        big(128, D), big(128, D), pltpu.VMEM((128, D), F32), big(4, 2, 128, D),
        pltpu.VMEM((4, 2, 128, D), F32), big(4, 128, D), big(4, 128, D), pltpu.VMEM((2, 64, D), F32),
        big(128, D), big(128, D), big(128, D), big(64, D), big(64, D), big(128, D), big(128, D),
        big(128, D), big(176, 264), big(HEAD, 176), pltpu.VMEM((128, 256), F32),
        *[big(n) for n in (D, D, D, D, D, D, 264, 384)],
        dma((SENDS,)), dma((COPIES,)), dma((13,)),
    ]
    return pl.pallas_call(
        kernel,
        out_shape=pltpu.VMEM((128, D), BF16),
        in_specs=[hbm] * 13,
        out_specs=vmem,
        scratch_shapes=scratch,
        compiler_params=pltpu.CompilerParams(
            collective_id=0, has_side_effects=True, vmem_limit_bytes=62 * 1024 * 1024
        ),
    )(
        tokens_in, ln1_gain, ln1_bias, proj_bias, ln2_gain, ln2_bias, fc2_bias, qkv_bias, fc1_bias,
        qkv_weight, proj_weight, fc1_weight, fc2_weight,
    )


def solution(mesh):
    in_specs = (
        P(("row", "col"), None), P(), P(), P("row", "col"), P("col"), P("col", "row"), P(),
        P(), P(), P("row", "col"), P("col"), P("row", "col"), P(),
    )
    return jax.shard_map(
        local, mesh=mesh, in_specs=in_specs, out_specs=P(("row", "col"), None), check_vma=False
    )
```
